32 devices in a mesh: groups: 2 (over y), expert: 8 (over z, x), mp: 2 (over core).
Axes of the slice: x: 2, y: 2, z: 4, core: 2. Of those that a mesh axis runs over, the one named last changes fastest.
Arguments:
- tokens: bfloat16 [64, 6144], P(('groups', 'expert', 'mp')), parts along dimension 0, may hold values from -6 to 6
- expert_ids: int32 [64, 2], P(('groups', 'expert', 'mp')), parts along dimension 0, may hold values from 0 to 3, all different within a row; in each aligned block of 2 rows (0 to 1, 2 to 3, ...) at most 2 rows name the same one
- mix_weights: float32 [64, 2], P(('groups', 'expert', 'mp')), parts along dimension 0, may hold values from 0.2 to 1
- w_gate: bfloat16 [6144, 32768], P(None, ('expert', 'mp')), may hold values from -0.078125 to 0.078125
- w_up: bfloat16 [6144, 32768], P(None, ('expert', 'mp')), may hold values from -0.078125 to 0.078125
- w_down: bfloat16 [32768, 6144], P(('expert', 'mp')), may hold values from -0.0625 to 0.0625
Outputs:
- combined: bfloat16 [64, 6144], P(('groups', 'expert', 'mp')), parts along dimension 0
The draws below stay inside these ranges and needn't reach their ends.
There are 2 independent parts, one for each index of `groups`. The reference program is written for one: setup_inputs(seed, part) draws one part's arguments, and reference() takes and returns one part's arrays. A program takes and returns all parts, laid end to end along the dimension named above; an argument that names none is the same for every part. Nothing has to cross between parts.
Inputs may be any that keep to these rules, and one draw needn't show every extreme that they name: `expert_ids`: each row names two different experts. Among the rows of one device no expert is named more than 2 times, and in every draw some device names some expert exactly 2 times.
All inputs are finite; a program needn't handle non-finite values.
Results may differ from the reference program's by a relative error of at most 0.0081.
Values may be sent and summed in bfloat16 or wider, within the bound.
A program may use at most 128 MiB of HBM per device.

```python
import math
import jax
import jax.numpy as jnp
import numpy as np

D = 6144
FF = 8192
EXPERTS = 4
TOK_DEV = 2
CAP = 2
TOKENS = 32


def shard_levels(rng, extent, shards, least, high):
    gain = 1.0
    for axis_at, blocks in shards:
        heights = jax.random.uniform(jax.random.fold_in(jax.random.fold_in(rng, 6), axis_at), (blocks,), jnp.float32, least / len(shards), high / len(shards))
        gain = gain * jnp.repeat(jnp.exp(heights), extent[axis_at] // blocks).reshape((-1,) + (1,) * (len(extent) - 1 - axis_at))
    return gain


def deal_out(own_key, own, number, rows, count, top, bound, slope):
    sequence = jax.random.permutation(own_key, count)
    crowded, ordinary = load_shares(count, rows * top, bound, slope, True), load_shares(count, rows * top, bound, slope, False)
    places = jnp.arange(count)

    def named(sizes, turn):
        used = int((sizes > 0).sum())
        fixed = max(1, used // 4)
        moved = fixed + (places - fixed + turn * (used - fixed)) % max(1, count - fixed)
        return jnp.zeros((count,), jnp.int32).at[sequence[jnp.where(places < fixed, places, moved)]].set(jnp.asarray(sizes, jnp.int32))

    sizes = jnp.where(number % 4 == 0, named(crowded, number // 4), named(ordinary, number - number // 4 - 1))
    mixed = jax.random.permutation(jax.random.fold_in(own, 3), count)
    source_of, sink = mixed[0:count // 2 * 2:2], mixed[1:count // 2 * 2:2]
    room = jnp.minimum(sizes[source_of] - 1, bound - sizes[sink]) // 2
    room = jnp.where((source_of == sequence[0]) | (sink == sequence[0]) | (sizes[sink] == 0), 0, jnp.maximum(room, 0))
    moved = jax.random.randint(jax.random.fold_in(own, 4), (count // 2,), 0, 1 << 20) % (room + 1)
    sizes = sizes.at[source_of].add(-moved).at[sink].add(moved)
    members = jnp.searchsorted(jnp.cumsum(sizes), jnp.arange(rows * top), side="right").astype(jnp.int32)
    listing = members.reshape(top, rows).T
    listing = listing[jax.random.permutation(jax.random.fold_in(own, 1), rows)]
    turn = jax.random.randint(jax.random.fold_in(own, 2), (rows, 1), 0, top)
    return jnp.take_along_axis(listing, (jnp.arange(top)[None, :] + turn) % top, axis=1)


def load_shares(amount, total, bound, skew, full):
    portions = [(1 << 20) // math.isqrt(rank ** skew) + 1 for rank in range(1, amount + 1)]
    largest = bound if full else min(bound, max(-(-total // amount), total * portions[0] // sum(portions)))
    least = 1 if total - largest >= amount - 1 else 0
    counts, rest = [largest] + [least] * (amount - 1), total - largest - least * (amount - 1)
    while rest > 0:
        free = [i for i in range(1, amount) if counts[i] < largest] or [i for i in range(1, amount) if counts[i] < bound]
        whole, left = sum([portions[i] for i in free]), rest
        for i in free:
            extra = min(bound - counts[i], max(1, left * portions[i] // whole), rest)
            counts[i] = counts[i] + extra
            rest = rest - extra
    return np.array(counts)


def centred(stream_key, dims, width, most, pieces=(), held_as=jnp.bfloat16):
    gain = shard_levels(stream_key, dims, pieces, -0.22, 0.18) if pieces else 1.0
    drawn = jax.random.normal(stream_key, dims, jnp.float32) * width * gain
    return jnp.minimum(jnp.maximum(drawn, -most), most).astype(held_as)


def setup_inputs(seed: int = 0, part: int = 0) -> dict:
    keys = jax.random.split(jax.random.key(seed), 7)
    part_splits = jax.random.split(jax.random.fold_in(keys[6], part), 7)
    tokens = centred(part_splits[0], (TOKENS, D), 1.0, 6.0, ((0, 16),))
    expert_ids_keys = jax.random.split(jax.random.fold_in(part_splits[1], 1), TOKENS // TOK_DEV)
    expert_ids_turns = jax.random.permutation(jax.random.fold_in(part_splits[1], 3), TOKENS // TOK_DEV)
    expert_ids = jax.vmap(lambda own, number: deal_out(jax.random.fold_in(part_splits[1], 2), own, number, TOK_DEV, EXPERTS, 2, CAP, 2))(expert_ids_keys, expert_ids_turns).reshape((TOKENS, 2))
    mix_weights = jnp.clip(0.2 + 0.8 * jax.random.uniform(part_splits[2], (TOKENS, 2), jnp.float32) ** shard_levels(part_splits[2], (TOKENS, 2), ((0, 16),), -0.2, 0.2), 0.2, 1.0)
    w_gate = centred(keys[3], (D, EXPERTS * FF), D ** -0.5, 0.078125, ((1, 16),))
    w_up = centred(keys[4], (D, EXPERTS * FF), D ** -0.5, 0.078125, ((1, 16),))
    w_down = centred(keys[5], (EXPERTS * FF, D), FF ** -0.5, 0.0625, ((0, 16),))
    return dict(tokens=tokens, expert_ids=expert_ids, mix_weights=mix_weights, w_gate=w_gate, w_up=w_up, w_down=w_down)


def reference(tokens, expert_ids, mix_weights, w_gate, w_up, w_down):
    summed = jnp.zeros((tokens.shape[0], D), jnp.float32)
    for expert in range(EXPERTS):
        start = expert * FF
        gate_part = jnp.dot(tokens, w_gate[:, start:start + FF], preferred_element_type=jnp.float32)
        up_part = jnp.dot(tokens, w_up[:, start:start + FF], preferred_element_type=jnp.float32)
        hidden = (jax.nn.silu(gate_part) * up_part).astype(jnp.bfloat16)
        output = jnp.dot(hidden, w_down[start:start + FF, :], preferred_element_type=jnp.float32)
        weight = jnp.sum(jnp.where(expert_ids == expert, mix_weights, jnp.zeros_like(mix_weights)), axis=1)
        summed = summed + weight[:, None] * output
    return summed.astype(jnp.bfloat16)
```

```python
import functools

import jax
import jax.numpy as jnp
from jax import lax
from jax.experimental import pallas as pl
from jax.experimental.pallas import tpu as pltpu
from jax.sharding import PartitionSpec as P

EXPERTS = 4
SLOT_BUDGET = 58 * 1024 * 1024
VMEM_LIMIT = 67043328
EARLY = 6
LAG = 2
MESH = pl.DeviceIdType.MESH


def block_of(extent, most):
    size = min(extent, most)
    while extent % size:
        size //= 2
    return size


def kernel(
    shards, cores, plan,
    ids_ref, mix_ref, tok_ref, gate_ref, up_ref, down_ref, out_ref,
    slots, arrived, rows_ref, hidden_ref, outbox, inbox,
    slot_sem, tok_send, tok_recv, own_sem, part_send, part_recv,
):
    kg, ng, kd, nd, depth = plan
    model_dim, units = gate_ref.shape
    count = shards * cores
    tok_rows = tok_ref.shape[0]
    rows = count * tok_rows
    k_blocks, n_blocks, out_blocks = model_dim // kg, units // ng, model_dim // nd
    first_total = n_blocks * k_blocks * 2
    total = first_total + out_blocks
    me = lax.axis_index("expert") * cores + lax.axis_index("mp")

    def where(peer):
        return {"expert": peer // cores, "mp": lax.rem(peer, cores)}

    def peer_at(step):
        return lax.rem(me + step, count)

    barrier = pltpu.get_barrier_semaphore()

    @pl.loop(1, count)
    def _(step):
        pl.semaphore_signal(barrier, inc=1, device_id=where(peer_at(step)), device_id_type=MESH)

    def gate_copy(c, source):
        pair = c // 2
        n, k = pair // k_blocks, lax.rem(pair, k_blocks)
        slot = lax.rem(c, depth)
        return pltpu.make_async_copy(
            source.at[pl.ds(pl.multiple_of(k * kg, kg), kg), pl.ds(pl.multiple_of(n * ng, ng), ng)],
            slots.at[slot, pl.ds(0, kg), pl.ds(0, ng)],
            slot_sem.at[slot],
        )

    def down_copy(c):
        slot = lax.rem(c, depth)
        col = (c - first_total) * nd
        return pltpu.make_async_copy(
            down_ref.at[:, pl.ds(pl.multiple_of(col, nd), nd)],
            slots.at[slot, pl.ds(0, kd), pl.ds(0, nd)],
            slot_sem.at[slot],
        )

    def start_chunk(c):
        odd = lax.rem(c, 2)

        @pl.when((c < first_total) & (odd == 0))
        def _():
            gate_copy(c, gate_ref).start()

        @pl.when((c < first_total) & (odd == 1))
        def _():
            gate_copy(c, up_ref).start()

        @pl.when((c >= first_total) & (c < total))
        def _():
            down_copy(c).start()

    early = min(EARLY, depth)

    @pl.loop(0, early)
    def _(c):
        start_chunk(c)

    own = pltpu.make_async_copy(tok_ref, arrived.at[me], own_sem)
    own.start()
    pl.semaphore_wait(barrier, count - 1)

    def token_copy(step):
        return pltpu.make_async_remote_copy(
            src_ref=tok_ref, dst_ref=arrived.at[me], send_sem=tok_send, recv_sem=tok_recv,
            device_id=where(peer_at(step)), device_id_type=MESH,
        )

    @pl.loop(1, count)
    def _(step):
        token_copy(step).start()

    @pl.loop(early, depth)
    def _(c):
        start_chunk(c)

    own.wait()
    others = arrived.at[pl.ds(0, count - 1)]
    pltpu.make_async_copy(others, others, tok_recv).wait()

    group = 16 // tok_rows

    @pl.loop(0, count // group)
    def _(g):
        pieces = [arrived[g * group + j] for j in range(group)]
        rows_ref[pl.ds(pl.multiple_of(g * 16, 16), 16), :] = jnp.concatenate(pieces, axis=0)

    @pl.loop(0, n_blocks)
    def _(n):
        sums = [jnp.zeros((rows, ng), jnp.float32), jnp.zeros((rows, ng), jnp.float32)]
        for k in range(k_blocks):
            for side in range(2):
                c = (n * k_blocks + k) * 2 + side
                slot = lax.rem(c, depth)
                gate_copy(c, (gate_ref, up_ref)[side]).wait()
                sums[side] = sums[side] + jnp.dot(
                    rows_ref[:, k * kg:(k + 1) * kg],
                    slots[slot, pl.ds(0, kg), pl.ds(0, ng)],
                    preferred_element_type=jnp.float32,
                )
                start_chunk(c + depth)
        hidden = (jax.nn.silu(sums[0]) * sums[1]).astype(jnp.bfloat16)
        hidden_ref[:, pl.ds(pl.multiple_of(n * ng, ng), ng)] = hidden

    def part_copy(block, step):
        cols = pl.ds(pl.multiple_of(block * nd, nd), nd)
        peer = peer_at(step)
        return pltpu.make_async_remote_copy(
            src_ref=outbox.at[peer, :, cols], dst_ref=inbox.at[me, :, cols],
            send_sem=part_send.at[block], recv_sem=part_recv.at[block],
            device_id=where(peer), device_id_type=MESH,
        )

    per = count // EXPERTS
    row_at = lax.broadcasted_iota(jnp.int32, (tok_rows, nd), 0)

    def combine(block):
        cols = pl.ds(pl.multiple_of(block * nd, nd), nd)
        landed = inbox.at[pl.ds(0, count - 1), :, cols]
        pltpu.make_async_copy(landed, landed, part_recv.at[block]).wait()
        result = jnp.zeros((tok_rows, nd), jnp.float32)
        for expert in range(EXPERTS):
            weight = jnp.zeros((tok_rows, nd), jnp.float32)
            for t in range(tok_rows):
                scale = jnp.float32(0.0)
                for k in range(ids_ref.shape[1]):
                    scale = scale + jnp.where(ids_ref[t, k] == expert, mix_ref[t, k], 0.0)
                weight = jnp.where(row_at == t, scale, weight)
            value = lax.fori_loop(
                0, per,
                lambda i, s: s + inbox[expert * per + i, :, cols].astype(jnp.float32),
                jnp.zeros((tok_rows, nd), jnp.float32),
                unroll=per <= 8,
            )
            result = result + weight * value
        out_ref[:, cols] = result.astype(out_ref.dtype)

    @pl.loop(0, out_blocks)
    def _(block):
        c = first_total + block
        cols = pl.ds(pl.multiple_of(block * nd, nd), nd)
        down_copy(c).wait()
        part = jnp.dot(
            hidden_ref[...], slots[lax.rem(c, depth), pl.ds(0, kd), pl.ds(0, nd)],
            preferred_element_type=jnp.float32,
        ).astype(jnp.bfloat16)
        start_chunk(c + depth)
        for p in range(count):
            outbox[p, :, cols] = part[p * tok_rows:(p + 1) * tok_rows, :]
        inbox[me, :, cols] = outbox[me, :, cols]

        @pl.loop(1, count)
        def _(step):
            part_copy(block, step).start()

        @pl.when(block >= LAG)
        def _():
            combine(block - LAG)

    @pl.loop(out_blocks - LAG, out_blocks)
    def _(block):
        combine(block)

    pltpu.make_async_copy(others, others, tok_send).wait()

    @pl.loop(0, out_blocks)
    def _(block):
        left = outbox.at[pl.ds(0, count - 1), :, pl.ds(pl.multiple_of(block * nd, nd), nd)]
        pltpu.make_async_copy(left, left, part_send.at[block]).wait()


def per_device(tokens, expert_ids, mix_weights, w_gate, w_up, w_down):
    shards, cores = lax.axis_size("expert"), lax.axis_size("mp")
    count = shards * cores
    tok_rows, model_dim = tokens.shape
    units = w_gate.shape[1]
    kg, ng = block_of(model_dim, 2048), block_of(units, 512)
    kd, nd = units, block_of(model_dim, 512)
    slot_shape = (max(kg, kd), max(ng, nd))
    chunks = (model_dim // kg) * (units // ng) * 2 + model_dim // nd
    kept = 4 * count * tok_rows * model_dim * 2
    depth = min(chunks, (SLOT_BUDGET - kept) // (slot_shape[0] * slot_shape[1] * 2))
    vmem = pl.BlockSpec(memory_space=pltpu.VMEM)
    smem = pl.BlockSpec(memory_space=pltpu.SMEM)
    hbm = pl.BlockSpec(memory_space=pl.ANY)
    boxes = (count, tok_rows, model_dim)
    return pl.pallas_call(
        functools.partial(kernel, shards, cores, (kg, ng, kd, nd, depth)),
        out_shape=jax.ShapeDtypeStruct((tok_rows, model_dim), jnp.bfloat16),
        in_specs=[smem, smem, vmem, hbm, hbm, hbm],
        out_specs=vmem,
        scratch_shapes=[
            pltpu.VMEM((depth, *slot_shape), jnp.bfloat16),
            pltpu.VMEM(boxes, jnp.bfloat16),
            pltpu.VMEM((count * tok_rows, model_dim), jnp.bfloat16),
            pltpu.VMEM((count * tok_rows, units), jnp.bfloat16),
            pltpu.VMEM(boxes, jnp.bfloat16),
            pltpu.VMEM(boxes, jnp.bfloat16),
            pltpu.SemaphoreType.DMA((depth,)),
            pltpu.SemaphoreType.DMA,
            pltpu.SemaphoreType.DMA,
            pltpu.SemaphoreType.DMA,
            pltpu.SemaphoreType.DMA((model_dim // nd,)),
            pltpu.SemaphoreType.DMA((model_dim // nd,)),
        ],
        compiler_params=pltpu.CompilerParams(
            collective_id=0, has_side_effects=True, vmem_limit_bytes=VMEM_LIMIT
        ),
    )(expert_ids, mix_weights, tokens, w_gate, w_up, w_down)


def solution(mesh):
    in_specs = (
        P(("groups", "expert", "mp"), None),
        P(("groups", "expert", "mp"), None),
        P(("groups", "expert", "mp"), None),
        P(None, ("expert", "mp")),
        P(None, ("expert", "mp")),
        P(("expert", "mp"), None),
    )
    out_specs = P(("groups", "expert", "mp"), None)
    return jax.shard_map(
        per_device, mesh=mesh, in_specs=in_specs, out_specs=out_specs, check_vma=False
    )
```

```python
import functools

import jax
import jax.numpy as jnp
from jax import lax
from jax.experimental import pallas as pl
from jax.experimental.pallas import tpu as pltpu
from jax.sharding import PartitionSpec as P

EXPERTS = 4
SLOT_BUDGET = 58 * 1024 * 1024
VMEM_LIMIT = 67043328
EARLY = 6
HOP = 1
LAG = 5
MESH = pl.DeviceIdType.MESH


def block_of(extent, most):
    size = min(extent, most)
    while extent % size:
        size //= 2
    return size


def kernel(
    shards, cores, plan,
    ids_ref, mix_ref, tok_ref, gate_ref, up_ref, down_ref, out_ref,
    slots, arrived, rows_ref, hidden_ref, outbox, corebox, sumbox, inbox,
    slot_sem, tok_send, tok_recv, own_sem, pass_send, pass_recv,
    core_send, core_recv, part_send, part_recv,
):
    kg, ng, kd, nd, depth = plan
    model_dim, units = gate_ref.shape
    count = shards * cores
    tok_rows = tok_ref.shape[0]
    rows = count * tok_rows
    k_blocks, n_blocks, out_blocks = model_dim // kg, units // ng, model_dim // nd
    first_total = n_blocks * k_blocks * 2
    total = first_total + out_blocks
    shard, core = lax.axis_index("expert"), lax.axis_index("mp")

    def shard_at(step):
        return lax.rem(shard + step, shards)

    def core_at(step):
        return lax.rem(core + step, cores)

    barrier = pltpu.get_barrier_semaphore()

    for step in range(1, cores):
        pl.semaphore_signal(barrier, inc=1, device_id={"mp": core_at(step)}, device_id_type=MESH)

    @pl.loop(1, shards)
    def _(step):
        pl.semaphore_signal(
            barrier, inc=1, device_id={"expert": shard_at(step)}, device_id_type=MESH
        )

    def gate_copy(c, source):
        pair = c // 2
        n, k = pair // k_blocks, lax.rem(pair, k_blocks)
        slot = lax.rem(c, depth)
        return pltpu.make_async_copy(
            source.at[pl.ds(pl.multiple_of(k * kg, kg), kg), pl.ds(pl.multiple_of(n * ng, ng), ng)],
            slots.at[slot, pl.ds(0, kg), pl.ds(0, ng)],
            slot_sem.at[slot],
        )

    def down_copy(c):
        slot = lax.rem(c, depth)
        col = (c - first_total) * nd
        return pltpu.make_async_copy(
            down_ref.at[:, pl.ds(pl.multiple_of(col, nd), nd)],
            slots.at[slot, pl.ds(0, kd), pl.ds(0, nd)],
            slot_sem.at[slot],
        )

    def start_chunk(c):
        odd = lax.rem(c, 2)

        @pl.when((c < first_total) & (odd == 0))
        def _():
            gate_copy(c, gate_ref).start()

        @pl.when((c < first_total) & (odd == 1))
        def _():
            gate_copy(c, up_ref).start()

        @pl.when((c >= first_total) & (c < total))
        def _():
            down_copy(c).start()

    early = min(EARLY, depth)

    @pl.loop(0, early)
    def _(c):
        start_chunk(c)

    own = pltpu.make_async_copy(tok_ref, arrived.at[core, shard], own_sem)
    own.start()
    pl.semaphore_wait(barrier, shards + cores - 2)

    def token_copy(step, source):
        return pltpu.make_async_remote_copy(
            src_ref=tok_ref, dst_ref=arrived.at[core, shard],
            send_sem=tok_send, recv_sem=tok_recv.at[source],
            device_id={"expert": shard_at(step)}, device_id_type=MESH,
        )

    def pass_on(source, step, from_ref):
        return pltpu.make_async_remote_copy(
            src_ref=from_ref, dst_ref=arrived.at[core, source],
            send_sem=pass_send, recv_sem=pass_recv,
            device_id={"mp": core_at(step)}, device_id_type=MESH,
        )

    @pl.loop(1, shards)
    def _(step):
        token_copy(step, shard).start()

    for step in range(1, cores):
        pass_on(shard, step, tok_ref).start()

    @pl.loop(early, depth)
    def _(c):
        start_chunk(c)

    @pl.loop(1, shards)
    def _(step):
        source = lax.rem(shard + shards - step, shards)
        token_copy(step, source).wait_recv()
        for other in range(1, cores):
            pass_on(source, other, arrived.at[core, source]).start()

    own.wait()
    for step in range(1, cores):
        whole = arrived.at[core_at(step)]
        pltpu.make_async_copy(whole, whole, pass_recv).wait()

    group = 16 // tok_rows

    @pl.loop(0, count // group)
    def _(g):
        flat = [g * group + j for j in range(group)]
        pieces = [arrived[i // shards, lax.rem(i, shards)] for i in flat]
        rows_ref[pl.ds(pl.multiple_of(g * 16, 16), 16), :] = jnp.concatenate(pieces, axis=0)

    @pl.loop(0, n_blocks)
    def _(n):
        sums = [jnp.zeros((rows, ng), jnp.float32), jnp.zeros((rows, ng), jnp.float32)]
        for k in range(k_blocks):
            for side in range(2):
                c = (n * k_blocks + k) * 2 + side
                slot = lax.rem(c, depth)
                gate_copy(c, (gate_ref, up_ref)[side]).wait()
                sums[side] = sums[side] + jnp.dot(
                    rows_ref[:, k * kg:(k + 1) * kg],
                    slots[slot, pl.ds(0, kg), pl.ds(0, ng)],
                    preferred_element_type=jnp.float32,
                )
                start_chunk(c + depth)
        hidden = (jax.nn.silu(sums[0]) * sums[1]).astype(jnp.bfloat16)
        hidden_ref[:, pl.ds(pl.multiple_of(n * ng, ng), ng)] = hidden

    def cols_of(block):
        return pl.ds(pl.multiple_of(block * nd, nd), nd)

    def core_copy(block, step):
        return pltpu.make_async_remote_copy(
            src_ref=outbox.at[core_at(step), :, :, cols_of(block)],
            dst_ref=corebox.at[core, :, :, cols_of(block)],
            send_sem=core_send.at[block], recv_sem=core_recv.at[block],
            device_id={"mp": core_at(step)}, device_id_type=MESH,
        )

    def part_copy(block, step):
        peer = shard_at(step)
        return pltpu.make_async_remote_copy(
            src_ref=sumbox.at[peer, :, cols_of(block)],
            dst_ref=inbox.at[shard, :, cols_of(block)],
            send_sem=part_send.at[block], recv_sem=part_recv.at[block],
            device_id={"expert": peer}, device_id_type=MESH,
        )

    def exchange(block):
        cols = cols_of(block)
        landed = corebox.at[pl.ds(0, cores - 1), :, :, cols]
        pltpu.make_async_copy(landed, landed, core_recv.at[block]).wait()

        def add_up(owner, carry):
            value = outbox[core, owner, :, cols].astype(jnp.float32)
            for step in range(1, cores):
                value = value + corebox[core_at(step), owner, :, cols].astype(jnp.float32)
            sumbox[owner, :, cols] = value.astype(jnp.bfloat16)
            return carry

        lax.fori_loop(0, shards, add_up, 0, unroll=shards <= 8)
        inbox[shard, :, cols] = sumbox[shard, :, cols]

        @pl.loop(1, shards)
        def _(step):
            part_copy(block, step).start()

    per = shards // EXPERTS
    row_at = lax.broadcasted_iota(jnp.int32, (tok_rows, nd), 0)

    def combine(block):
        cols = cols_of(block)
        landed = inbox.at[pl.ds(0, shards - 1), :, cols]
        pltpu.make_async_copy(landed, landed, part_recv.at[block]).wait()
        result = jnp.zeros((tok_rows, nd), jnp.float32)
        for expert in range(EXPERTS):
            weight = jnp.zeros((tok_rows, nd), jnp.float32)
            for t in range(tok_rows):
                scale = jnp.float32(0.0)
                for k in range(ids_ref.shape[1]):
                    scale = scale + jnp.where(ids_ref[t, k] == expert, mix_ref[t, k], 0.0)
                weight = jnp.where(row_at == t, scale, weight)
            value = lax.fori_loop(
                0, per,
                lambda i, s: s + inbox[expert * per + i, :, cols].astype(jnp.float32),
                jnp.zeros((tok_rows, nd), jnp.float32),
                unroll=per <= 8,
            )
            result = result + weight * value
        out_ref[:, cols] = result.astype(out_ref.dtype)

    @pl.loop(0, out_blocks)
    def _(block):
        c = first_total + block
        cols = cols_of(block)
        down_copy(c).wait()
        part = jnp.dot(
            hidden_ref[...], slots[lax.rem(c, depth), pl.ds(0, kd), pl.ds(0, nd)],
            preferred_element_type=jnp.float32,
        ).astype(jnp.bfloat16)
        start_chunk(c + depth)
        for p in range(count):
            outbox[p // shards, p % shards, :, cols] = part[p * tok_rows:(p + 1) * tok_rows, :]
        for step in range(1, cores):
            core_copy(block, step).start()

        @pl.when(block >= HOP)
        def _():
            exchange(block - HOP)

        @pl.when(block >= LAG)
        def _():
            combine(block - LAG)

    for block in range(max(out_blocks - HOP, 0), out_blocks):
        exchange(block)
    for block in range(max(out_blocks - LAG, 0), out_blocks):
        combine(block)

    tokens_out = arrived.at[0, pl.ds(0, shards - 1)]
    pltpu.make_async_copy(tokens_out, tokens_out, tok_send).wait()
    passed = arrived.at[pl.ds(0, cores - 1)]
    pltpu.make_async_copy(passed, passed, pass_send).wait()

    @pl.loop(0, out_blocks)
    def _(block):
        left = outbox.at[pl.ds(0, cores - 1), :, :, cols_of(block)]
        pltpu.make_async_copy(left, left, core_send.at[block]).wait()
        left = sumbox.at[pl.ds(0, shards - 1), :, cols_of(block)]
        pltpu.make_async_copy(left, left, part_send.at[block]).wait()


def per_device(tokens, expert_ids, mix_weights, w_gate, w_up, w_down):
    shards, cores = lax.axis_size("expert"), lax.axis_size("mp")
    count = shards * cores
    tok_rows, model_dim = tokens.shape
    units = w_gate.shape[1]
    kg, ng = block_of(model_dim, 2048), block_of(units, 512)
    kd, nd = units, block_of(model_dim, 512)
    slot_shape = (max(kg, kd), max(ng, nd))
    chunks = (model_dim // kg) * (units // ng) * 2 + model_dim // nd
    kept = 5 * count * tok_rows * model_dim * 2
    depth = min(chunks, (SLOT_BUDGET - kept) // (slot_shape[0] * slot_shape[1] * 2))
    vmem = pl.BlockSpec(memory_space=pltpu.VMEM)
    smem = pl.BlockSpec(memory_space=pltpu.SMEM)
    hbm = pl.BlockSpec(memory_space=pl.ANY)
    boxes = (cores, shards, tok_rows, model_dim)
    return pl.pallas_call(
        functools.partial(kernel, shards, cores, (kg, ng, kd, nd, depth)),
        out_shape=jax.ShapeDtypeStruct((tok_rows, model_dim), jnp.bfloat16),
        in_specs=[smem, smem, vmem, hbm, hbm, hbm],
        out_specs=vmem,
        scratch_shapes=[
            pltpu.VMEM((depth, *slot_shape), jnp.bfloat16),
            pltpu.VMEM(boxes, jnp.bfloat16),
            pltpu.VMEM((count * tok_rows, model_dim), jnp.bfloat16),
            pltpu.VMEM((count * tok_rows, units), jnp.bfloat16),
            pltpu.VMEM(boxes, jnp.bfloat16),
            pltpu.VMEM(boxes, jnp.bfloat16),
            pltpu.VMEM(boxes[1:], jnp.bfloat16),
            pltpu.VMEM(boxes[1:], jnp.bfloat16),
            pltpu.SemaphoreType.DMA((depth,)),
            pltpu.SemaphoreType.DMA,
            pltpu.SemaphoreType.DMA((shards,)),
            pltpu.SemaphoreType.DMA,
            pltpu.SemaphoreType.DMA,
            pltpu.SemaphoreType.DMA,
            *[pltpu.SemaphoreType.DMA((model_dim // nd,))] * 4,
        ],
        compiler_params=pltpu.CompilerParams(
            collective_id=0, has_side_effects=True, vmem_limit_bytes=VMEM_LIMIT
        ),
    )(expert_ids, mix_weights, tokens, w_gate, w_up, w_down)


def solution(mesh):
    in_specs = (
        P(("groups", "expert", "mp"), None),
        P(("groups", "expert", "mp"), None),
        P(("groups", "expert", "mp"), None),
        P(None, ("expert", "mp")),
        P(None, ("expert", "mp")),
        P(("expert", "mp"), None),
    )
    out_specs = P(("groups", "expert", "mp"), None)
    return jax.shard_map(
        per_device, mesh=mesh, in_specs=in_specs, out_specs=out_specs, check_vma=False
    )
```

```python
import functools

import jax
import jax.numpy as jnp
from jax import lax
from jax.experimental import pallas as pl
from jax.experimental.pallas import tpu as pltpu
from jax.sharding import PartitionSpec as P

EXPERTS = 4
SLOT_BUDGET = 58 * 1024 * 1024
VMEM_LIMIT = 67043328
EARLY = 6
HOP = 2
LAG = 8
MESH = pl.DeviceIdType.MESH


def block_of(extent, most):
    size = min(extent, most)
    while extent % size:
        size //= 2
    return size


def kernel(
    shards, cores, plan,
    ids_ref, mix_ref, tok_ref, gate_ref, up_ref, down_ref, out_ref,
    slots, arrived, rows_ref, hidden_ref, outbox, corebox, sumbox, inbox,
    slot_sem, tok_send, tok_recv, own_sem, pass_send, pass_recv,
    core_send, core_recv, part_send, part_recv,
):
    kg, ng, kd, nd, depth = plan
    model_dim, units = gate_ref.shape
    count = shards * cores
    tok_rows = tok_ref.shape[0]
    rows = count * tok_rows
    k_blocks, n_blocks, out_blocks = model_dim // kg, units // ng, model_dim // nd
    first_total = n_blocks * k_blocks * 2
    total = first_total + out_blocks
    shard, core = lax.axis_index("expert"), lax.axis_index("mp")

    def shard_at(step):
        return lax.rem(shard + step, shards)

    def core_at(step):
        return lax.rem(core + step, cores)

    barrier = pltpu.get_barrier_semaphore()

    for step in range(1, cores):
        pl.semaphore_signal(barrier, inc=1, device_id={"mp": core_at(step)}, device_id_type=MESH)

    @pl.loop(1, shards)
    def _(step):
        pl.semaphore_signal(
            barrier, inc=1, device_id={"expert": shard_at(step)}, device_id_type=MESH
        )

    def gate_copy(c, source):
        pair = c // 2
        n, k = pair // k_blocks, lax.rem(pair, k_blocks)
        slot = lax.rem(c, depth)
        return pltpu.make_async_copy(
            source.at[pl.ds(pl.multiple_of(k * kg, kg), kg), pl.ds(pl.multiple_of(n * ng, ng), ng)],
            slots.at[slot, pl.ds(0, kg), pl.ds(0, ng)],
            slot_sem.at[slot],
        )

    def down_copy(c):
        slot = lax.rem(c, depth)
        col = (c - first_total) * nd
        return pltpu.make_async_copy(
            down_ref.at[:, pl.ds(pl.multiple_of(col, nd), nd)],
            slots.at[slot, pl.ds(0, kd), pl.ds(0, nd)],
            slot_sem.at[slot],
        )

    def start_chunk(c):
        odd = lax.rem(c, 2)

        @pl.when((c < first_total) & (odd == 0))
        def _():
            gate_copy(c, gate_ref).start()

        @pl.when((c < first_total) & (odd == 1))
        def _():
            gate_copy(c, up_ref).start()

        @pl.when((c >= first_total) & (c < total))
        def _():
            down_copy(c).start()

    early = min(EARLY, depth)

    @pl.loop(0, early)
    def _(c):
        start_chunk(c)

    own = pltpu.make_async_copy(tok_ref, arrived.at[core, shard], own_sem)
    own.start()
    pl.semaphore_wait(barrier, shards + cores - 2)

    def token_copy(step, source):
        return pltpu.make_async_remote_copy(
            src_ref=tok_ref, dst_ref=arrived.at[core, shard],
            send_sem=tok_send, recv_sem=tok_recv.at[source],
            device_id={"expert": shard_at(step)}, device_id_type=MESH,
        )

    def pass_on(source, step, from_ref):
        return pltpu.make_async_remote_copy(
            src_ref=from_ref, dst_ref=arrived.at[core, source],
            send_sem=pass_send, recv_sem=pass_recv,
            device_id={"mp": core_at(step)}, device_id_type=MESH,
        )

    @pl.loop(1, shards)
    def _(step):
        token_copy(step, shard).start()

    for step in range(1, cores):
        pass_on(shard, step, tok_ref).start()

    @pl.loop(early, depth)
    def _(c):
        start_chunk(c)

    @pl.loop(1, shards)
    def _(step):
        source = lax.rem(shard + shards - step, shards)
        token_copy(step, source).wait_recv()
        for other in range(1, cores):
            pass_on(source, other, arrived.at[core, source]).start()

    own.wait()
    for step in range(1, cores):
        whole = arrived.at[core_at(step)]
        pltpu.make_async_copy(whole, whole, pass_recv).wait()

    group = 16 // tok_rows

    @pl.loop(0, count // group)
    def _(g):
        flat = [g * group + j for j in range(group)]
        pieces = [arrived[i // shards, lax.rem(i, shards)] for i in flat]
        rows_ref[pl.ds(pl.multiple_of(g * 16, 16), 16), :] = jnp.concatenate(pieces, axis=0)

    @pl.loop(0, n_blocks)
    def _(n):
        sums = [jnp.zeros((rows, ng), jnp.float32), jnp.zeros((rows, ng), jnp.float32)]
        for k in range(k_blocks):
            for side in range(2):
                c = (n * k_blocks + k) * 2 + side
                slot = lax.rem(c, depth)
                gate_copy(c, (gate_ref, up_ref)[side]).wait()
                sums[side] = sums[side] + jnp.dot(
                    rows_ref[:, k * kg:(k + 1) * kg],
                    slots[slot, pl.ds(0, kg), pl.ds(0, ng)],
                    preferred_element_type=jnp.float32,
                )
                start_chunk(c + depth)
        hidden = (jax.nn.silu(sums[0]) * sums[1]).astype(jnp.bfloat16)
        hidden_ref[:, pl.ds(pl.multiple_of(n * ng, ng), ng)] = hidden

    def cols_of(block):
        return pl.ds(pl.multiple_of(block * nd, nd), nd)

    def core_copy(block, step):
        return pltpu.make_async_remote_copy(
            src_ref=outbox.at[core_at(step), :, cols_of(block)],
            dst_ref=corebox.at[core, :, cols_of(block)],
            send_sem=core_send.at[block], recv_sem=core_recv.at[block],
            device_id={"mp": core_at(step)}, device_id_type=MESH,
        )

    def part_copy(block, step):
        peer = shard_at(step)
        return pltpu.make_async_remote_copy(
            src_ref=sumbox.at[peer, :, cols_of(block)],
            dst_ref=inbox.at[shard, :, cols_of(block)],
            send_sem=part_send.at[block], recv_sem=part_recv.at[block],
            device_id={"expert": peer}, device_id_type=MESH,
        )

    def exchange(block):
        cols = cols_of(block)
        landed = corebox.at[pl.ds(0, cores - 1), :, cols]
        pltpu.make_async_copy(landed, landed, core_recv.at[block]).wait()

        value = outbox[core, :, cols].astype(jnp.float32)
        for step in range(1, cores):
            value = value + corebox[core_at(step), :, cols].astype(jnp.float32)
        value = value.astype(jnp.bfloat16)
        for owner in range(shards):
            sumbox[owner, :, cols] = value[owner * tok_rows:(owner + 1) * tok_rows, :]
        inbox[shard, :, cols] = sumbox[shard, :, cols]

        @pl.loop(1, shards)
        def _(step):
            part_copy(block, step).start()

    per = shards // EXPERTS
    row_at = lax.broadcasted_iota(jnp.int32, (tok_rows, nd), 0)

    def combine(block):
        cols = cols_of(block)
        landed = inbox.at[pl.ds(0, shards - 1), :, cols]
        pltpu.make_async_copy(landed, landed, part_recv.at[block]).wait()
        result = jnp.zeros((tok_rows, nd), jnp.float32)
        for expert in range(EXPERTS):
            weight = jnp.zeros((tok_rows, nd), jnp.float32)
            for t in range(tok_rows):
                scale = jnp.float32(0.0)
                for k in range(ids_ref.shape[1]):
                    scale = scale + jnp.where(ids_ref[t, k] == expert, mix_ref[t, k], 0.0)
                weight = jnp.where(row_at == t, scale, weight)
            value = lax.fori_loop(
                0, per,
                lambda i, s: s + inbox[expert * per + i, :, cols].astype(jnp.float32),
                jnp.zeros((tok_rows, nd), jnp.float32),
                unroll=per <= 8,
            )
            result = result + weight * value
        out_ref[:, cols] = result.astype(out_ref.dtype)

    @pl.loop(0, out_blocks)
    def _(block):
        c = first_total + block
        cols = cols_of(block)
        down_copy(c).wait()
        part = jnp.dot(
            hidden_ref[...], slots[lax.rem(c, depth), pl.ds(0, kd), pl.ds(0, nd)],
            preferred_element_type=jnp.float32,
        ).astype(jnp.bfloat16)
        start_chunk(c + depth)
        half = shards * tok_rows
        for side in range(cores):
            outbox[side, :, cols] = part[side * half:(side + 1) * half, :]
        for step in range(1, cores):
            core_copy(block, step).start()

        @pl.when(block >= HOP)
        def _():
            exchange(block - HOP)

        @pl.when(block >= LAG)
        def _():
            combine(block - LAG)

    for block in range(max(out_blocks - HOP, 0), out_blocks):
        exchange(block)
    for block in range(max(out_blocks - LAG, 0), out_blocks):
        combine(block)

    tokens_out = arrived.at[0, pl.ds(0, shards - 1)]
    pltpu.make_async_copy(tokens_out, tokens_out, tok_send).wait()
    passed = arrived.at[pl.ds(0, cores - 1)]
    pltpu.make_async_copy(passed, passed, pass_send).wait()

    @pl.loop(0, out_blocks)
    def _(block):
        left = outbox.at[pl.ds(0, cores - 1), :, cols_of(block)]
        pltpu.make_async_copy(left, left, core_send.at[block]).wait()
        left = sumbox.at[pl.ds(0, shards - 1), :, cols_of(block)]
        pltpu.make_async_copy(left, left, part_send.at[block]).wait()


def per_device(tokens, expert_ids, mix_weights, w_gate, w_up, w_down):
    shards, cores = lax.axis_size("expert"), lax.axis_size("mp")
    count = shards * cores
    tok_rows, model_dim = tokens.shape
    units = w_gate.shape[1]
    kg, ng = block_of(model_dim, 2048), block_of(units, 512)
    kd, nd = units, block_of(model_dim, 512)
    slot_shape = (max(kg, kd), max(ng, nd))
    chunks = (model_dim // kg) * (units // ng) * 2 + model_dim // nd
    kept = 5 * count * tok_rows * model_dim * 2
    depth = min(chunks, (SLOT_BUDGET - kept) // (slot_shape[0] * slot_shape[1] * 2))
    vmem = pl.BlockSpec(memory_space=pltpu.VMEM)
    smem = pl.BlockSpec(memory_space=pltpu.SMEM)
    hbm = pl.BlockSpec(memory_space=pl.ANY)
    boxes = (cores, shards, tok_rows, model_dim)
    halves = (cores, shards * tok_rows, model_dim)
    return pl.pallas_call(
        functools.partial(kernel, shards, cores, (kg, ng, kd, nd, depth)),
        out_shape=jax.ShapeDtypeStruct((tok_rows, model_dim), jnp.bfloat16),
        in_specs=[smem, smem, vmem, hbm, hbm, hbm],
        out_specs=vmem,
        scratch_shapes=[
            pltpu.VMEM((depth, *slot_shape), jnp.bfloat16),
            pltpu.VMEM(boxes, jnp.bfloat16),
            pltpu.VMEM((count * tok_rows, model_dim), jnp.bfloat16),
            pltpu.VMEM((count * tok_rows, units), jnp.bfloat16),
            pltpu.VMEM(halves, jnp.bfloat16),
            pltpu.VMEM(halves, jnp.bfloat16),
            pltpu.VMEM(boxes[1:], jnp.bfloat16),
            pltpu.VMEM(boxes[1:], jnp.bfloat16),
            pltpu.SemaphoreType.DMA((depth,)),
            pltpu.SemaphoreType.DMA,
            pltpu.SemaphoreType.DMA((shards,)),
            pltpu.SemaphoreType.DMA,
            pltpu.SemaphoreType.DMA,
            pltpu.SemaphoreType.DMA,
            *[pltpu.SemaphoreType.DMA((model_dim // nd,))] * 4,
        ],
        compiler_params=pltpu.CompilerParams(
            collective_id=0, has_side_effects=True, vmem_limit_bytes=VMEM_LIMIT
        ),
    )(expert_ids, mix_weights, tokens, w_gate, w_up, w_down)


def solution(mesh):
    in_specs = (
        P(("groups", "expert", "mp"), None),
        P(("groups", "expert", "mp"), None),
        P(("groups", "expert", "mp"), None),
        P(None, ("expert", "mp")),
        P(None, ("expert", "mp")),
        P(("expert", "mp"), None),
    )
    out_specs = P(("groups", "expert", "mp"), None)
    return jax.shard_map(
        per_device, mesh=mesh, in_specs=in_specs, out_specs=out_specs, check_vma=False
    )
```
